32 devices in a mesh: gx: 8 (over z, x), gy: 4 (over y, core).
Axes of the slice: x: 2, y: 2, z: 4, core: 2. Of those that a mesh axis runs over, the one named last changes fastest.
Arguments:
- tokens: bfloat16 [256, 8192], P(None, 'gx'), may hold values from -16 to 16
- attn_gain: bfloat16 [8192], P('gx'), may hold values from 0.25 to 1.75
- qkv_weight: bfloat16 [8192, 10240], P('gx', 'gy'), may hold values from -0.0625 to 0.0625
- cache_keys: bfloat16 [256, 8, 512, 128], P('gx', 'gy'), may hold values from -160 to 160
- cache_values: bfloat16 [256, 8, 512, 128], P('gx', 'gy'), may hold values from -6 to 6
- lengths: int32 [256], replicated, may hold values from 1 to 512
- live_mask: int32 [256], replicated, may hold values 0 or 1
- out_weight: bfloat16 [8192, 8192], P('gy', 'gx'), may hold values from -0.0625 to 0.0625
- mlp_gain: bfloat16 [8192], P('gx'), may hold values from 0.25 to 1.75
- gate_weight: bfloat16 [8192, 28672], P('gx', 'gy'), may hold values from -0.0625 to 0.0625
- up_weight: bfloat16 [8192, 28672], P('gx', 'gy'), may hold values from -0.0625 to 0.0625
- down_weight: bfloat16 [28672, 8192], P('gy', 'gx'), may hold values from -0.03125 to 0.03125
Outputs:
- updated: bfloat16 [256, 8192], P('gy', 'gx')
The draws below stay inside these ranges and needn't reach their ends.
All inputs are finite; a program needn't handle non-finite values.
Results may differ from the reference program's by a relative error of at most 0.0095.
Values may be sent and summed in bfloat16 or wider, within the bound.
A program may use at most 128 MiB of HBM per device.

```python
import jax
import jax.numpy as jnp
from jax import lax

D = 8192
H = 64
KVH = 8
HD = 128
FF = 28672
CACHE = 512
BATCH = 256


def draw_tokens(key, part):
    key_cols, key_base, key_rows, key_common = jax.random.split(jax.random.fold_in(key, 11), 4)
    block_width = D // 32
    col_scale = jnp.exp(jax.random.uniform(key_cols, (32,), jnp.float32, -0.9, 0.9))
    col_scale = jnp.repeat(col_scale, block_width)[None, :]
    base_draw = jax.random.normal(key_base, (BATCH, D), jnp.float32)
    values = base_draw * col_scale
    return jnp.clip(values, -16.0, 16.0).astype(jnp.bfloat16)


def draw_cache_keys(key, part):
    key_base, key_pick, key_sign = jax.random.split(jax.random.fold_in(key, 23), 3)
    dims_all = (BATCH, KVH, CACHE, HD)
    values = jnp.clip(jax.random.normal(key_base, dims_all, jnp.float32), -6.0, 6.0)
    return values.astype(jnp.bfloat16)


def plant(array, key, low, largest):
    index_at = [jax.random.randint(jax.random.fold_in(key, axis), (), 0, length) for axis, length in enumerate(array.shape)]
    longest = array.shape.index(max(array.shape))
    beside = index_at[:longest] + [(index_at[longest] + 1) % array.shape[longest]] + index_at[longest + 1:]
    return array.at[tuple(index_at)].set(low).at[tuple(beside)].set(largest)


def block_scale(key, shape, shards, least, largest):
    level = 1.0
    for axis_at, parts in shards:
        draws = jax.random.uniform(jax.random.fold_in(jax.random.fold_in(key, 6), axis_at), (parts,), jnp.float32, least / len(shards), largest / len(shards))
        level = level * jnp.repeat(jnp.exp(draws), shape[axis_at] // parts).reshape((-1,) + (1,) * (len(shape) - 1 - axis_at))
    return level


def noise(stream_key, dims, width, bound, shards=(), held_as=jnp.bfloat16):
    values = jax.random.normal(stream_key, dims, jnp.float32) * width
    if len(shards) > 0:
        values = block_scale(stream_key, dims, shards, -0.22, 0.18) * values
    return jnp.clip(values, min=-bound, max=bound).astype(held_as)


def setup_inputs(seed: int = 0) -> dict:
    splits = jax.random.split(jax.random.key(seed), 13)
    tokens = draw_tokens(jax.random.fold_in(splits[12], 71), 0)
    attn_gain = jnp.clip(1.0 + 0.15 * jax.random.normal(splits[1], (D,), jnp.float32), 0.25, 1.75).astype(jnp.bfloat16)
    qkv_weight = noise(splits[2], (D, KVH * (H // KVH + 2) * HD), D ** -0.5, 0.0625, ((0, 8), (1, 4)))
    cache_keys = draw_cache_keys(jax.random.fold_in(splits[12], 71), 0)
    cache_values = noise(splits[4], (BATCH, KVH, CACHE, HD), 1.0, 6.0, ((0, 8), (1, 4)))
    lengths = plant(jax.random.randint(splits[5], (BATCH,), 1, CACHE + 1), jax.random.fold_in(splits[5], 1), 1, CACHE).astype(jnp.int32)
    live_mask = plant((jax.random.randint(splits[6], (BATCH,), 0, 4) < 3).astype(jnp.int32), jax.random.fold_in(splits[6], 1), 0, 1)
    out_weight = noise(splits[7], (H * HD, D), (H * HD) ** -0.5, 0.0625, ((0, 4), (1, 8)))
    mlp_gain = jnp.clip(1.0 + 0.15 * jax.random.normal(splits[8], (D,), jnp.float32), 0.25, 1.75).astype(jnp.bfloat16)
    gate_weight = noise(splits[9], (D, FF), D ** -0.5, 0.0625, ((0, 8), (1, 4)))
    up_weight = noise(splits[10], (D, FF), D ** -0.5, 0.0625, ((0, 8), (1, 4)))
    down_weight = noise(splits[11], (FF, D), FF ** -0.5, 0.03125, ((0, 4), (1, 8)))
    return {"tokens": tokens, "attn_gain": attn_gain, "qkv_weight": qkv_weight, "cache_keys": cache_keys, "cache_values": cache_values, "lengths": lengths, "live_mask": live_mask, "out_weight": out_weight, "mlp_gain": mlp_gain, "gate_weight": gate_weight, "up_weight": up_weight, "down_weight": down_weight}


ROPE_BASE = 500000.0
NORM_EPS = 1e-05
MASKED = -1e+30

def rotate_pairs(vectors, positions):
    half_width = vectors.shape[-1] // 2
    index_float = jnp.arange(half_width).astype(jnp.float32)
    inv_freq = jnp.exp(index_float * (-2.0 * jnp.log(ROPE_BASE) / vectors.shape[-1]))
    angles = positions.astype(jnp.float32)[:, None] * inv_freq[None, :]
    cosine = jnp.cos(angles)[:, None, :]
    sine_part = jnp.sin(angles)[:, None, :]
    low_half = vectors[..., :half_width]
    high_half = vectors[..., half_width:]
    return jnp.concatenate((low_half * cosine - high_half * sine_part, high_half * cosine + low_half * sine_part), axis=-1)

def attend_group(query_rows, fresh_key_rows, new_values, grouped_key_rows, grouped_value_rows, lengths):
    score_scale = query_rows.shape[-1] ** (-0.5)
    stored_entries = jnp.einsum('whj,wpj->whp', query_rows.astype(jnp.float32), grouped_key_rows.astype(jnp.float32)) * score_scale
    valid = jnp.arange(grouped_key_rows.shape[1])[None, None, :] < lengths[:, None, None]
    stored_entries = jnp.where(valid, stored_entries, MASKED)
    self_token = jnp.einsum('rnj,rj->rn', query_rows.astype(jnp.float32), fresh_key_rows.astype(jnp.float32)) * score_scale
    peak = jnp.maximum(lax.optimization_barrier(jnp.max(stored_entries, axis=-1)), self_token)
    attention_probs = jnp.where(valid, jnp.exp(stored_entries - peak[..., None]), 0.0).astype(jnp.bfloat16)
    own_weight = jnp.exp(self_token - peak).astype(jnp.bfloat16)
    totals = lax.optimization_barrier(jnp.sum(attention_probs.astype(jnp.float32), axis=-1)) + own_weight.astype(jnp.float32)
    blended_values = jnp.einsum('zcx,zxr->zcr', attention_probs.astype(jnp.float32), grouped_value_rows.astype(jnp.float32))
    blended_values = blended_values + own_weight.astype(jnp.float32)[..., None] * new_values.astype(jnp.float32)[:, None, :]
    return (blended_values / totals[..., None]).astype(jnp.bfloat16)

def reference(tokens, attn_gain, qkv_weight, cache_keys, cache_values, lengths, live_mask, out_weight, mlp_gain, gate_weight, up_weight, down_weight):
    rows_all = tokens.shape[0]
    per_kv = H // KVH
    wide_in = tokens.astype(jnp.float32)
    attn_scale = lax.rsqrt(lax.optimization_barrier(jnp.sum(wide_in * wide_in, axis=1)) / D + NORM_EPS)
    scaled = (wide_in * attn_gain.astype(jnp.float32)).astype(jnp.bfloat16)
    projected = jnp.dot(scaled, qkv_weight, preferred_element_type=jnp.float32) * attn_scale[:, None]
    projected = projected.reshape(rows_all, KVH, per_kv + 2, HD)
    query_rows = rotate_pairs(projected[:, :, :per_kv].reshape(rows_all, H, HD), lengths)
    query_rows = query_rows.astype(jnp.bfloat16).reshape(rows_all, KVH, per_kv, HD)
    fresh_key_rows = rotate_pairs(projected[:, :, per_kv], lengths).astype(jnp.bfloat16)
    new_values = projected[:, :, per_kv + 1].astype(jnp.bfloat16)

    def one_group(group_index):
        query_group = lax.dynamic_index_in_dim(query_rows, group_index, 1, keepdims=False)
        key_new = lax.dynamic_index_in_dim(fresh_key_rows, group_index, 1, keepdims=False)
        value_new = lax.dynamic_index_in_dim(new_values, group_index, 1, keepdims=False)
        grouped_key_rows = lax.dynamic_index_in_dim(cache_keys, group_index, 1, keepdims=False)
        grouped_value_rows = lax.dynamic_index_in_dim(cache_values, group_index, 1, keepdims=False)
        return attend_group(query_group, key_new, value_new, grouped_key_rows, grouped_value_rows, lengths)
    grouped = lax.map(one_group, jnp.arange(KVH).astype(jnp.int32))
    attn = jnp.transpose(grouped, (1, 0, 2, 3)).reshape(rows_all, H * HD)
    attn_proj = jnp.dot(attn, out_weight, preferred_element_type=jnp.float32)
    alive_col = live_mask.astype(jnp.float32)[:, None]
    residual = (wide_in + alive_col * attn_proj).astype(jnp.bfloat16)
    resid_wide = residual.astype(jnp.float32)
    mlp_scale = lax.rsqrt(lax.optimization_barrier(jnp.sum(resid_wide * resid_wide, axis=1)) / D + NORM_EPS)
    mlp_in = (resid_wide * mlp_gain.astype(jnp.float32)).astype(jnp.bfloat16)
    gate_sum = jnp.dot(mlp_in, gate_weight, preferred_element_type=jnp.float32) * mlp_scale[:, None]
    up_sum = jnp.dot(mlp_in, up_weight, preferred_element_type=jnp.float32) * mlp_scale[:, None]
    hidden = (jax.nn.silu(gate_sum) * up_sum).astype(jnp.bfloat16)
    down_sum = jnp.dot(hidden, down_weight, preferred_element_type=jnp.float32)
    return (resid_wide + alive_col * down_sum).astype(jnp.bfloat16)
```

```python
import functools

import jax
import jax.numpy as jnp
from jax import lax
from jax.experimental import pallas as pl
from jax.experimental.pallas import tpu as pltpu
from jax.sharding import PartitionSpec as P

D = 8192
H = 64
KVH = 8
HD = 128


ROPE_BASE = 500000.0
NORM_EPS = 1e-05
MASKED = -1e30


def rotate_pairs(vectors, positions):
    half_width = vectors.shape[-1] // 2
    index_float = jnp.arange(half_width).astype(jnp.float32)
    inv_freq = jnp.exp(index_float * (-2.0 * jnp.log(ROPE_BASE) / vectors.shape[-1]))
    angles = positions.astype(jnp.float32)[:, None] * inv_freq[None, :]
    cosine = jnp.cos(angles)[:, None, :]
    sine_part = jnp.sin(angles)[:, None, :]
    low_half = vectors[..., :half_width]
    high_half = vectors[..., half_width:]
    return jnp.concatenate(
        (low_half * cosine - high_half * sine_part, high_half * cosine + low_half * sine_part),
        axis=-1,
    )


def make_heads(projected, square_rows, positions, groups, per_kv):
    row_count = projected.shape[0]
    attn_scale = lax.rsqrt(square_rows / D + NORM_EPS)
    shaped = (projected * attn_scale[:, None]).reshape(row_count, groups, per_kv + 2, HD)
    query_rows = rotate_pairs(
        shaped[:, :, :per_kv].reshape(row_count, groups * per_kv, HD), positions
    )
    query_rows = query_rows.astype(jnp.bfloat16).reshape(row_count, groups, per_kv, HD)
    fresh_key_rows = rotate_pairs(shaped[:, :, per_kv], positions).astype(jnp.bfloat16)
    new_values = shaped[:, :, per_kv + 1].astype(jnp.bfloat16)
    return (query_rows, fresh_key_rows, new_values)


def attend(query_rows, fresh_key_rows, new_values, cache_keys, cache_values, lengths):
    score_scale = query_rows.shape[-1] ** (-0.5)
    stored_entries = (
        jnp.einsum("bgqd,bgld->bgql", query_rows, cache_keys, preferred_element_type=jnp.float32)
        * score_scale
    )
    places = jnp.arange(cache_keys.shape[2])
    valid = places[None, None, None, :] < lengths[:, None, None, None]
    stored_entries = jnp.where(valid, stored_entries, MASKED)
    self_token = (
        jnp.einsum("bgqd,bgd->bgq", query_rows, fresh_key_rows, preferred_element_type=jnp.float32)
        * score_scale
    )
    peak = jnp.maximum(jnp.max(stored_entries, axis=-1), self_token)
    attention_probs = jnp.where(valid, jnp.exp(stored_entries - peak[..., None]), 0.0).astype(
        jnp.bfloat16
    )
    weight_sum = jnp.sum(attention_probs.astype(jnp.float32), axis=-1)
    blended_values = jnp.einsum(
        "bgql,bgld->bgqd", attention_probs, cache_values, preferred_element_type=jnp.float32
    )
    own_weight = jnp.exp(self_token - peak).astype(jnp.bfloat16).astype(jnp.float32)
    totals = weight_sum + own_weight
    blended_values = (
        blended_values + own_weight[..., None] * new_values.astype(jnp.float32)[:, :, None, :]
    )
    return (blended_values / totals[..., None]).astype(jnp.bfloat16)


def greet(axis, n, me):
    barrier = pltpu.get_barrier_semaphore()
    for k in range(1, n):
        pl.semaphore_signal(
            barrier,
            inc=1,
            device_id={axis: lax.rem(me + k, n)},
            device_id_type=pl.DeviceIdType.MESH,
        )
    pl.semaphore_wait(barrier, n - 1)


def exchange_kernel(axis, n, m, *refs):
    sources, slots = refs[:m], refs[m : 2 * m]
    send_sem, recv_sem = refs[2 * m :]
    me = lax.axis_index(axis)
    greet(axis, n, me)
    copies = []
    for k in range(1, n):
        target = lax.rem(me + k, n)
        for i in range(m):
            copies.append(
                pltpu.make_async_remote_copy(
                    src_ref=sources[i].at[target],
                    dst_ref=slots[i].at[k - 1],
                    send_sem=send_sem.at[i, k - 1],
                    recv_sem=recv_sem.at[i, k - 1],
                    device_id={axis: target},
                    device_id_type=pl.DeviceIdType.MESH,
                )
            )
            copies[-1].start()
    for copy in copies:
        copy.wait()


def sum_scatter(arrays, axis, collective_id):
    n = lax.axis_size(axis)
    me = lax.axis_index(axis)
    m = len(arrays)
    blocked = [a.reshape(n, a.shape[0] // n, a.shape[1]) for a in arrays]
    sent = sum((n - 1) * b[0].size * b.dtype.itemsize for b in blocked)
    received = pl.pallas_call(
        functools.partial(exchange_kernel, axis, n, m),
        out_shape=[jax.ShapeDtypeStruct((n - 1,) + b.shape[1:], b.dtype) for b in blocked],
        in_specs=[pl.BlockSpec(memory_space=pl.ANY)] * m,
        out_specs=[pl.BlockSpec(memory_space=pl.ANY)] * m,
        scratch_shapes=[
            pltpu.SemaphoreType.DMA((m, n - 1)),
            pltpu.SemaphoreType.DMA((m, n - 1)),
        ],
        cost_estimate=pl.CostEstimate(flops=0, bytes_accessed=20 * sent, transcendentals=0),
        compiler_params=pltpu.CompilerParams(collective_id=collective_id, has_side_effects=True),
    )(*blocked)
    totals = []
    for b, r in zip(blocked, received):
        own = lax.dynamic_index_in_dim(b, me, 0, keepdims=False).astype(jnp.float32)
        totals.append(own + jnp.sum(r.astype(jnp.float32), axis=0))
    return totals


def gather_kernel(axis, n, source, gathered, send_sem, recv_sem, own_sem):
    me = lax.axis_index(axis)
    greet(axis, n, me)
    copies = []
    for k in range(1, n):
        copies.append(
            pltpu.make_async_remote_copy(
                src_ref=source,
                dst_ref=gathered.at[me],
                send_sem=send_sem.at[k - 1],
                recv_sem=recv_sem.at[k - 1],
                device_id={axis: lax.rem(me + k, n)},
                device_id_type=pl.DeviceIdType.MESH,
            )
        )
        copies[-1].start()
    own = pltpu.make_async_copy(source, gathered.at[me], own_sem)
    own.start()
    own.wait()
    for copy in copies:
        copy.wait()


def gather_rows(array, axis, collective_id):
    n = lax.axis_size(axis)
    sent = (n - 1) * array.size * array.dtype.itemsize
    gathered = pl.pallas_call(
        functools.partial(gather_kernel, axis, n),
        out_shape=jax.ShapeDtypeStruct((n,) + array.shape, array.dtype),
        in_specs=[pl.BlockSpec(memory_space=pltpu.VMEM)],
        out_specs=pl.BlockSpec(memory_space=pl.ANY),
        scratch_shapes=[
            pltpu.SemaphoreType.DMA((n - 1,)),
            pltpu.SemaphoreType.DMA((n - 1,)),
            pltpu.SemaphoreType.DMA,
        ],
        cost_estimate=pl.CostEstimate(flops=0, bytes_accessed=20 * sent, transcendentals=0),
        compiler_params=pltpu.CompilerParams(collective_id=collective_id, has_side_effects=True),
    )(array)
    return gathered.reshape(n * array.shape[0], array.shape[1])


def relay_kernel(axis, n, source, gathered, send_sem, recv_sem, side_send, side_recv, own_sem):
    m = n // 2
    reach = m // 2
    half = source.shape[0] // 2
    me = lax.axis_index(axis)
    z, x = me // 2, lax.rem(me, 2)
    partner = z * 2 + 1 - x
    sides = (lax.rem(z + 1, m) * 2 + x, lax.rem(z + m - 1, m) * 2 + x)
    barrier = pltpu.get_barrier_semaphore()
    for device in (partner,) + sides:
        pl.semaphore_signal(
            barrier, inc=1, device_id={axis: device}, device_id_type=pl.DeviceIdType.MESH
        )
    pl.semaphore_wait(barrier, 3)

    def hop(way, c, h):
        back = h - 1 if way == 0 else m - h + 1
        slot = lax.rem(z + m - back, m) * 2 + (x if c == 0 else 1 - x)
        src = source if h == 1 and c == 0 else gathered.at[slot]
        dst = gathered.at[slot]
        if h == reach:
            rows = pl.ds(way * half, half)
            src, dst = src.at[rows], dst.at[rows]
        return pltpu.make_async_remote_copy(
            src_ref=src,
            dst_ref=dst,
            send_sem=send_sem.at[way, c, h - 1],
            recv_sem=recv_sem.at[way, c, h - 1],
            device_id={axis: sides[way]},
            device_id_type=pl.DeviceIdType.MESH,
        )

    hops = {(w, c, h): hop(w, c, h) for w in (0, 1) for c in (0, 1) for h in range(1, reach + 1)}
    across = pltpu.make_async_remote_copy(
        src_ref=source,
        dst_ref=gathered.at[me],
        send_sem=side_send,
        recv_sem=side_recv,
        device_id={axis: partner},
        device_id_type=pl.DeviceIdType.MESH,
    )
    across.start()
    for w in (0, 1):
        hops[w, 0, 1].start()
    own = pltpu.make_async_copy(source, gathered.at[me], own_sem)
    own.start()
    across.wait_recv()
    for w in (0, 1):
        hops[w, 1, 1].start()
    for h in range(1, reach + 1):
        for c in (0, 1):
            for w in (0, 1):
                hops[w, c, h].wait_recv()
                if h < reach:
                    hops[w, c, h + 1].start()
    own.wait()
    across.wait_send()
    for copy in hops.values():
        copy.wait_send()


def relay_rows(array, axis, collective_id):
    n = lax.axis_size(axis)
    if n % 4 or n < 8:
        return gather_rows(array, axis, collective_id)
    sent = (n - 1) * array.size * array.dtype.itemsize
    ways = (2, 2, n // 4)
    gathered = pl.pallas_call(
        functools.partial(relay_kernel, axis, n),
        out_shape=jax.ShapeDtypeStruct((n,) + array.shape, array.dtype),
        in_specs=[pl.BlockSpec(memory_space=pltpu.VMEM)],
        out_specs=pl.BlockSpec(memory_space=pl.ANY),
        scratch_shapes=[
            pltpu.SemaphoreType.DMA(ways),
            pltpu.SemaphoreType.DMA(ways),
            pltpu.SemaphoreType.DMA,
            pltpu.SemaphoreType.DMA,
            pltpu.SemaphoreType.DMA,
        ],
        cost_estimate=pl.CostEstimate(flops=0, bytes_accessed=20 * sent, transcendentals=0),
        compiler_params=pltpu.CompilerParams(collective_id=collective_id, has_side_effects=True),
    )(array)
    return gathered.reshape(n * array.shape[0], array.shape[1])


def spread(column):
    return jnp.broadcast_to(column[:, None], (column.shape[0], 128))


def per_device(
    tokens,
    attn_gain,
    qkv_weight,
    cache_keys,
    cache_values,
    lengths,
    live_mask,
    out_weight,
    mlp_gain,
    gate_weight,
    up_weight,
    down_weight,
):
    batch_size = tokens.shape[0]
    local_rows = batch_size // lax.axis_size("gx")
    groups = cache_keys.shape[1]
    per_kv = H // KVH
    row_start = lax.axis_index("gx") * local_rows
    wide_in = tokens.astype(jnp.float32)
    scaled = (wide_in * attn_gain.astype(jnp.float32)).astype(jnp.bfloat16)
    squares = jnp.sum(wide_in * wide_in, axis=1)
    partial_sum = jnp.dot(scaled, qkv_weight, preferred_element_type=jnp.float32)
    own_proj, own_squares = sum_scatter(
        [partial_sum.astype(jnp.bfloat16), spread(squares)], "gx", 0
    )
    own_lengths = lax.dynamic_slice_in_dim(lengths, row_start, local_rows, 0)
    query_rows, fresh_key_rows, new_values = make_heads(
        own_proj, own_squares[:, 0], own_lengths, groups, per_kv
    )
    attn = attend(query_rows, fresh_key_rows, new_values, cache_keys, cache_values, own_lengths)
    attn = attn.reshape(local_rows, groups * per_kv * HD)
    proj_part = jnp.dot(
        relay_rows(attn, "gx", 1), out_weight, preferred_element_type=jnp.float32
    )
    out_rows = batch_size // lax.axis_size("gy")
    out_start = lax.axis_index("gy") * out_rows
    (attn_proj,) = sum_scatter([proj_part.astype(jnp.bfloat16)], "gy", 2)
    alive_rows = lax.dynamic_slice_in_dim(live_mask, out_start, out_rows, 0)
    alive_rows = alive_rows.astype(jnp.float32)[:, None]
    token_rows = lax.dynamic_slice_in_dim(tokens, out_start, out_rows, 0).astype(jnp.float32)
    resid_rows = (token_rows + alive_rows * attn_proj).astype(jnp.bfloat16)
    resid_wide = gather_rows(resid_rows, "gy", 3).astype(jnp.float32)
    mlp_in = (resid_wide * mlp_gain.astype(jnp.float32)).astype(jnp.bfloat16)
    resid_squares = jnp.sum(resid_wide * resid_wide, axis=1)
    gate_part = jnp.dot(mlp_in, gate_weight, preferred_element_type=jnp.float32)
    up_part = jnp.dot(mlp_in, up_weight, preferred_element_type=jnp.float32)
    gate_sum, up_sum, own_all = sum_scatter(
        [gate_part.astype(jnp.bfloat16), up_part.astype(jnp.bfloat16), spread(resid_squares)],
        "gx",
        4,
    )
    mlp_scale = lax.rsqrt(own_all[:, :1] / D + NORM_EPS)
    hidden_share = (jax.nn.silu(gate_sum * mlp_scale) * (up_sum * mlp_scale)).astype(jnp.bfloat16)
    down_full = jnp.dot(
        relay_rows(hidden_share, "gx", 5), down_weight, preferred_element_type=jnp.float32
    )
    (down_sum,) = sum_scatter([down_full.astype(jnp.bfloat16)], "gy", 6)
    return (resid_rows.astype(jnp.float32) + alive_rows * down_sum).astype(jnp.bfloat16)


def solution(mesh):
    return jax.shard_map(
        per_device,
        mesh=mesh,
        in_specs=(
            P(None, "gx"),
            P("gx"),
            P("gx", "gy"),
            P("gx", "gy", None, None),
            P("gx", "gy", None, None),
            P(),
            P(),
            P("gy", "gx"),
            P("gx"),
            P("gx", "gy"),
            P("gx", "gy"),
            P("gy", "gx"),
        ),
        out_specs=P("gy", "gx"),
        check_vma=False,
    )
```
